128 devices in a mesh: section: 2 (over core), tp: 8 (over z_lo, x), fsdp: 8 (over z_hi, y).
Axes of the slice: x: 4, y: 4, z: 4 (z_hi: 2, z_lo: 2; z = z_hi * 2 + z_lo), core: 2. Of those that a mesh axis runs over, the one named last changes fastest.
Arguments:
- normed: bfloat16 [2, 1024, 4608], P('section', 'tp', 'fsdp'), may hold values from -6 to 6
- cotangent: bfloat16 [2, 1024, 4608], P('section', 'tp', 'fsdp'), may hold values from -6 to 6
- w_gate: bfloat16 [2, 4608, 18432], P('section', 'fsdp', 'tp'), may hold values from -0.09375 to 0.09375
- w_up: bfloat16 [2, 4608, 18432], P('section', 'fsdp', 'tp'), may hold values from -0.09375 to 0.09375
- w_down: bfloat16 [2, 4608, 18432], P('section', 'fsdp', 'tp'), may hold values from -0.046875 to 0.046875
Outputs:
- passed: bfloat16 [2, 1024, 4608], P('section', 'tp', 'fsdp')
- grad_gate: bfloat16 [2, 4608, 18432], P('section', 'fsdp', 'tp')
- grad_up: bfloat16 [2, 4608, 18432], P('section', 'fsdp', 'tp')
- grad_down: bfloat16 [2, 4608, 18432], P('section', 'fsdp', 'tp')
The draws below stay inside these ranges and needn't reach their ends.
All inputs are finite; a program needn't handle non-finite values.
Results may differ from the reference program's by a relative error of at most 0.012.
Values may be sent and summed in bfloat16 or wider, within the bound.
No kernel may reach another device: no remote copies, remote signals or barrier semaphores. Data moves between devices by JAX's collectives and lax.ppermute only.
A program may use at most 192 MiB of HBM per device.

```python
import math
import jax
import jax.numpy as jnp

D = 4608
FF = 18432
TOKENS = 1024


def block_scale(rng, shape, cuts, low, top_value):
    def one(axis_at, blocks):
        draws = jax.random.uniform(jax.random.fold_in(jax.random.fold_in(rng, 6), axis_at), (blocks,), jnp.float32, low / len(cuts), top_value / len(cuts))
        return jnp.repeat(jnp.exp(draws), shape[axis_at] // blocks).reshape((-1,) + (1,) * (len(shape) - axis_at - 1))

    level = one(*cuts[0])
    for cut in cuts[1:]:
        level = level * one(*cut)
    return level


def centred(stream_key, shape, width, limit, shards=(), dtype=jnp.bfloat16):
    drawn = width * jax.random.normal(stream_key, shape, jnp.float32)
    if shards:
        drawn = drawn * block_scale(stream_key, shape, shards, -0.22, 0.18)
    return jnp.clip(drawn, -limit, limit).astype(dtype)


def setup_inputs(seed: int = 0) -> dict:
    key_list = jax.random.split(jax.random.key(seed), 6)
    normed = centred(key_list[0], (2, TOKENS, D), 1.0, 6.0, ((0, 2), (1, 8), (2, 8)))
    cotangent = centred(key_list[1], (2, TOKENS, D), 1.0, 6.0, ((0, 2), (1, 8), (2, 8)))
    w_gate = centred(key_list[2], (2, D, FF), D ** -0.5, 0.09375, ((0, 2), (1, 8), (2, 8)))
    w_up = centred(key_list[3], (2, D, FF), D ** -0.5, 0.09375, ((0, 2), (1, 8), (2, 8)))
    w_down = centred(key_list[4], (2, D, FF), FF ** -0.5, 0.046875, ((0, 2), (1, 8), (2, 8)))
    return {"normed": normed, "cotangent": cotangent, "w_gate": w_gate, "w_up": w_up, "w_down": w_down}


def activate(gate, up, back):
    coeff = math.sqrt(2.0 / math.pi)
    inner = jnp.tanh(coeff * (gate + 0.044715 * gate * gate * gate))
    act = 0.5 * gate * (1.0 + inner)
    slope = 0.5 * (1.0 + inner) + 0.5 * gate * (1.0 - inner * inner) * coeff * (1.0 + 3.0 * 0.044715 * gate * gate)
    hidden = (act * up).astype(jnp.bfloat16)
    d_gate = (back * up * slope).astype(jnp.bfloat16)
    d_up = (back * act).astype(jnp.bfloat16)
    return (hidden, d_gate, d_up)

def layer_back(rows, cot, wgate, wup, wdown):
    gate = jnp.dot(rows, wgate, preferred_element_type=jnp.float32)
    up = jnp.dot(rows, wup, preferred_element_type=jnp.float32)
    back = jnp.dot(cot, wdown, preferred_element_type=jnp.float32)
    hidden, d_gate, d_up = activate(gate, up, back)
    scale = 1.0 / math.sqrt(TOKENS)
    g_gate = (jnp.dot(rows.T, d_gate, preferred_element_type=jnp.float32) * scale).astype(jnp.bfloat16)
    g_up = (jnp.dot(rows.T, d_up, preferred_element_type=jnp.float32) * scale).astype(jnp.bfloat16)
    g_down = (jnp.dot(cot.T, hidden, preferred_element_type=jnp.float32) * scale).astype(jnp.bfloat16)
    branch = jnp.dot(d_gate, wgate.T, preferred_element_type=jnp.float32) + jnp.dot(d_up, wup.T, preferred_element_type=jnp.float32)
    handed = (cot.astype(jnp.float32) + branch).astype(jnp.bfloat16)
    return (handed, g_gate, g_up, g_down)

def reference(normed, cotangent, w_gate, w_up, w_down):
    first = layer_back(normed[0], cotangent[0], w_gate[0], w_up[0], w_down[0])
    second = layer_back(normed[1], cotangent[1], w_gate[1], w_up[1], w_down[1])
    passed = jnp.stack([second[0], first[0]])
    grad_gate = jnp.stack([first[1], second[1]])
    grad_up = jnp.stack([first[2], second[2]])
    grad_down = jnp.stack([first[3], second[3]])
    return (passed, grad_gate, grad_up, grad_down)
```

```python
import math

import jax
import jax.numpy as jnp
from jax import lax
from jax.experimental import pallas as pl
from jax.experimental.pallas import tpu as pltpu
from jax.sharding import PartitionSpec as P

TILE = 256
ROWS = 128
PART = 16
F32 = jnp.float32
BF16 = jnp.bfloat16

ROOM = pltpu.CompilerParams(vmem_limit_bytes=16 * 1024 * 1024)


def along_ring(v, axis, step):
    pairs = [(o * 4 + i, o * 4 + (i + step) % 4) for o in range(2) for i in range(4)]
    return lax.ppermute(v, axis, pairs)


def across(v, axis):
    return lax.ppermute(v, axis, [(i, (i + 4) % 8) for i in range(8)])


def added(*parts):
    total = parts[0].astype(F32)
    for p in parts[1:]:
        total = total + p.astype(F32)
    return total


def stacked(normed, cotangent):
    def kernel(n_ref, c_ref, out, cot):
        out[0] = n_ref[...].T
        rows = c_ref[...].T
        out[1] = rows
        cot[...] = rows

    depth, rows = normed.shape
    return pl.pallas_call(
        kernel,
        out_shape=[
            jax.ShapeDtypeStruct((2, rows, depth), BF16),
            jax.ShapeDtypeStruct((rows, depth), BF16),
        ],
        compiler_params=ROOM,
        name="stacked",
    )(normed, cotangent)


def gathered(own):
    left = along_ring(own, "tp", 1)
    right = along_ring(own, "tp", -1)
    other = across(own, "tp")
    far0 = along_ring(left[:1], "tp", 1)
    far1 = along_ring(right[1:], "tp", -1)
    oleft = along_ring(other, "tp", 1)
    oright = along_ring(other, "tp", -1)
    far = jnp.concatenate((far0, far1), axis=0)
    ofar = across(far, "tp")
    return [own, right, far, left, other, oright, ofar, oleft]


def project(pieces, owner, rows, weights, blocks, first, count, tile):
    depth = weights[0].shape[0]
    fresh = pieces is not None

    def kernel(*refs):
        if fresh:
            own_ref, ins = refs[0], refs[1:9]
            wg, wu, wd, rows_ref = refs[9:13]
            outs = refs[13:]

            @pl.when(pl.program_id(0) == 0)
            def _():
                for b in range(8):
                    at = pl.multiple_of(own_ref[b] * PART, PART)
                    for p in range(8):
                        lo = b * ROWS + p * PART
                        rows_ref[:, lo : lo + PART, :] = ins[p][:, pl.ds(at, PART), :]
        else:
            rows_ref, wg, wu, wd = refs[:4]
            outs = refs[4:]
        for w, (weight, which) in enumerate(((wg, 0), (wu, 0), (wd, 1))):
            left = rows_ref[which, blocks[0] * ROWS : (blocks[-1] + 1) * ROWS]
            out = jnp.dot(left, weight[...], preferred_element_type=F32).astype(BF16)
            for i in range(len(blocks)):
                outs[i][w] = out[i * ROWS : (i + 1) * ROWS]

    wspec = pl.BlockSpec((depth, tile), lambda j, *_: (0, first + j))
    rows_spec = pl.BlockSpec((2, 8 * ROWS, depth), lambda j, *_: (0, 0, 0))
    out_shape = [jax.ShapeDtypeStruct((3, ROWS, count * tile), BF16)] * len(blocks)
    out_specs = [pl.BlockSpec((3, ROWS, tile), lambda j, *_: (0, 0, j))] * len(blocks)
    if fresh:
        in_specs = [pl.BlockSpec((2, ROWS, depth), lambda j, *_: (0, 0, 0))] * 8 + [wspec] * 3
        out_shape = [jax.ShapeDtypeStruct((2, 8 * ROWS, depth), BF16)] + out_shape
        out_specs = [rows_spec] + out_specs
        args = (owner, *pieces, *weights)
    else:
        in_specs = [rows_spec] + [wspec] * 3
        args = (rows, *weights)
    return pl.pallas_call(
        kernel,
        out_shape=out_shape,
        grid_spec=pltpu.PrefetchScalarGridSpec(
            num_scalar_prefetch=1 if fresh else 0,
            grid=(count,),
            in_specs=in_specs,
            out_specs=out_specs,
        ),
        cost_estimate=pl.CostEstimate(
            flops=2 * len(blocks) * ROWS * depth * 3 * count * tile,
            bytes_accessed=2 * 3 * count * tile * (depth + len(blocks) * ROWS),
            transcendentals=0,
        ),
        compiler_params=ROOM,
    )(*args)


def flipped(rows):
    def kernel(rows_ref, out):
        for side in range(2):
            out[side] = rows_ref[side].T

    return pl.pallas_call(
        kernel,
        out_shape=jax.ShapeDtypeStruct((2, rows.shape[2], rows.shape[1]), BF16),
        cost_estimate=pl.CostEstimate(
            flops=10**8, bytes_accessed=4 * rows.size, transcendentals=0
        ),
        compiler_params=ROOM,
        name="flip",
    )(rows)


def reduced_ring_first(p):
    r1 = along_ring(p[2][1], "fsdp", 1)
    r0 = along_ring(p[2][0], "fsdp", -1)
    d1 = along_ring(p[3][1], "fsdp", -1)
    d0 = along_ring(p[1][0], "fsdp", 1)
    m1 = along_ring(added(p[1][1], r1).astype(BF16), "fsdp", 1)
    m0 = along_ring(added(p[3][0], r0).astype(BF16), "fsdp", -1)
    z = across(added(p[0][1], d1, m1).astype(BF16), "fsdp")
    return added(p[0][0], d0, m0, z)


def reduced_pair_first(p):
    half = p[0][0].shape[1] // 2
    z = {k: across(p[k][1], "fsdp") for k in (2, 1, 3, 0)}

    def low(k, *more):
        return added(p[k][0][:, :half], z[k][:, :half], *more).astype(BF16)

    def high(k, *more):
        return added(p[k][0][:, half:], z[k][:, half:], *more).astype(BF16)

    ra = along_ring(low(2), "fsdp", 1)
    rb = along_ring(high(2), "fsdp", -1)
    db = along_ring(high(1), "fsdp", 1)
    da = along_ring(low(3), "fsdp", -1)
    ma = along_ring(low(1, ra), "fsdp", 1)
    mb = along_ring(high(3, rb), "fsdp", -1)
    return added(p[0][0], z[0]) + jnp.concatenate((added(da, ma), added(db, mb)), axis=1)


def activate(sums):
    gate, up, back = sums[0], sums[1], sums[2]
    coeff = math.sqrt(2.0 / math.pi)
    inner = jnp.tanh(coeff * (gate + 0.044715 * gate * gate * gate))
    act = 0.5 * gate * (1.0 + inner)
    slope = 0.5 * (1.0 + inner) + 0.5 * gate * (1.0 - inner * inner) * coeff * (
        1.0 + 3.0 * 0.044715 * gate * gate
    )
    hidden = (act * up).astype(BF16)
    d_gate = (back * up * slope).astype(BF16)
    d_up = (back * act).astype(BF16)
    return jnp.stack((hidden, d_gate, d_up))


def spread_pair_first(own):
    z = across(own, "fsdp")
    fm = along_ring(own, "fsdp", 1)
    fp = along_ring(own, "fsdp", -1)
    gp = along_ring(z, "fsdp", -1)
    gm = along_ring(z, "fsdp", 1)
    f2 = along_ring(fm, "fsdp", 1)
    g2 = along_ring(gp, "fsdp", -1)
    return [[own], [z], [fp], [gp], [fm], [gm], [f2], [g2]]


def spread_ring_first(own):
    half = ROWS // 2
    fm = along_ring(own, "fsdp", 1)
    fp = along_ring(own, "fsdp", -1)
    z0 = across(own, "fsdp")
    fa = along_ring(fm[:, :half], "fsdp", 1)
    fb = along_ring(fp[:, half:], "fsdp", -1)
    z1 = across(fp, "fsdp")
    z3 = across(fm, "fsdp")
    za = across(fa, "fsdp")
    zb = across(fb, "fsdp")
    return [[own], [z0], [fp], [z1], [fm], [z3], [fa, fb], [za, zb]]


def flat(blocks):
    return [p for b in blocks for p in b]


def held(weights):
    def kernel(wu, wd, out):
        for i in range(8):
            out[i] = 0

    return pl.pallas_call(
        kernel,
        out_shape=jax.ShapeDtypeStruct((8,), jnp.int32),
        in_specs=[pl.BlockSpec(memory_space=pltpu.VMEM)] * 2,
        out_specs=pl.BlockSpec(memory_space=pltpu.SMEM),
        compiler_params=ROOM,
        name="held",
    )(*weights)


def part_specs(parts):
    return [pl.BlockSpec((3, p.shape[1], TILE), lambda j: (0, 0, j)) for p in parts]


SIDES = ((1, 0), (2, 0), (0, 1))


def products(sides_ref, parts, span):
    for plane, side in SIDES:
        right = jnp.concatenate([r[plane] for r in parts], axis=0)
        yield jnp.dot(sides_ref[side, :, span], right, preferred_element_type=F32)


def weight_sums(parts, sides, count):
    depth = sides.shape[1]
    tokens = sum(p.shape[1] for p in parts)

    def kernel(sides_ref, *refs):
        for out, value in zip(refs[-3:], products(sides_ref, refs[:-3], slice(0, tokens))):
            out[...] = value

    return pl.pallas_call(
        kernel,
        out_shape=[jax.ShapeDtypeStruct((depth, count * TILE), F32)] * 3,
        grid=(count,),
        in_specs=[pl.BlockSpec(sides.shape, lambda j: (0, 0, 0))] + part_specs(parts),
        out_specs=[pl.BlockSpec((depth, TILE), lambda j: (0, j))] * 3,
        cost_estimate=pl.CostEstimate(
            flops=2 * tokens * depth * 3 * count * TILE,
            bytes_accessed=2 * 3 * count * TILE * (2 * depth + tokens),
            transcendentals=0,
        ),
        compiler_params=ROOM,
    )(sides, *parts)


def weight_grads(parts, sides, sums, first, count, columns, scale, earlier):
    depth = sides.shape[1]
    n = len(parts)
    tokens = sum(p.shape[1] for p in parts)
    span = slice(sides.shape[2] - tokens, sides.shape[2])

    def kernel(sides_ref, *refs):
        for total, out, value in zip(refs[:3], refs[-3:], products(sides_ref, refs[3 : 3 + n], span)):
            out[...] = ((total[...] + value) * scale).astype(BF16)

    more = [] if earlier is None else list(earlier)
    return pl.pallas_call(
        kernel,
        out_shape=[jax.ShapeDtypeStruct((depth, columns), BF16)] * 3,
        grid=(count,),
        in_specs=[pl.BlockSpec(sides.shape, lambda j: (0, 0, 0))]
        + [pl.BlockSpec((depth, TILE), lambda j: (0, j))] * 3
        + part_specs(parts)
        + [pl.BlockSpec(memory_space=pl.ANY)] * len(more),
        out_specs=[pl.BlockSpec((depth, TILE), lambda j: (0, first + j))] * 3,
        input_output_aliases={4 + n + i: i for i in range(len(more))},
        cost_estimate=pl.CostEstimate(
            flops=2 * tokens * depth * 3 * count * TILE,
            bytes_accessed=2 * 3 * count * TILE * (3 * depth + tokens),
            transcendentals=0,
        ),
        compiler_params=ROOM,
    )(sides, *sums, *parts, *more)


def input_grad(parts_a, parts_b, weights, n_a, n_b, earlier, final):
    depth = weights[0].shape[0]
    na, nb = len(parts_a), len(parts_b)
    rows = sum(p.shape[1] for p in parts_a)
    before = 0 if earlier is None else earlier.shape[0]
    held = (before + rows) // ROWS
    count = n_a + n_b

    def kernel(*refs):
        wg, wu = refs[:2]
        ins_a, ins_b = refs[2 : 2 + na], refs[2 + na : 2 + na + nb]
        outs, total = refs[2 + na + nb + (before > 0) : -1], refs[-1]
        j = pl.program_id(0)

        def product(ins):
            acc = None
            for plane, weight in ((1, wg), (2, wu)):
                left = jnp.concatenate([r[plane] for r in ins], axis=0)
                more = lax.dot_general(
                    left, weight[...], (((1,), (1,)), ((), ())), preferred_element_type=F32
                )
                acc = more if acc is None else acc + more
            return acc

        @pl.when(j == 0)
        def _():
            total[...] = product(ins_a)

        @pl.when(jnp.logical_and(j > 0, j < n_a))
        def _():
            total[...] += product(ins_a)

        @pl.when(j >= n_a)
        def _():
            total[...] += product(ins_b)

        @pl.when(j == count - 1)
        def _():
            if not final:
                outs[0][...] = total[...].astype(BF16)
                return
            for i in range(held):
                for p in range(8):
                    lo = i * ROWS + p * PART
                    if lo < before:
                        value = refs[2 + na + nb][lo : lo + PART]
                    else:
                        value = total[lo - before : lo - before + PART].astype(BF16)
                    outs[p % 4][p // 4, i * PART : (i + 1) * PART] = value

    in_specs = [pl.BlockSpec((depth, TILE), lambda j: (0, j))] * 2
    in_specs += [
        pl.BlockSpec((3, p.shape[1], TILE), lambda j: (0, 0, jnp.minimum(j, n_a - 1)))
        for p in parts_a
    ]
    in_specs += [
        pl.BlockSpec((3, p.shape[1], TILE), lambda j: (0, 0, jnp.maximum(j - n_a, 0)))
        for p in parts_b
    ]
    args = (*weights, *parts_a, *parts_b)
    if before:
        in_specs.append(pl.BlockSpec(earlier.shape, lambda j: (0, 0)))
        args = (*args, earlier)
    if final:
        lengths = (2, held * PART, depth)
        out_shape = [jax.ShapeDtypeStruct(lengths, BF16)] * 4
        out_specs = [pl.BlockSpec(lengths, lambda j: (0, 0, 0))] * 4
    else:
        out_shape = [jax.ShapeDtypeStruct((rows, depth), BF16)]
        out_specs = [pl.BlockSpec((rows, depth), lambda j: (0, 0))]
    return pl.pallas_call(
        kernel,
        out_shape=out_shape,
        grid=(count,),
        in_specs=in_specs,
        out_specs=out_specs,
        scratch_shapes=[pltpu.VMEM((rows, depth), F32)],
        cost_estimate=pl.CostEstimate(
            flops=2 * rows * depth * 2 * count * TILE,
            bytes_accessed=2 * 2 * count * TILE * (depth + rows),
            transcendentals=0,
        ),
        compiler_params=ROOM,
    )(*args)


def to_other(v, a, b):
    pairs = [
        (s * 8 + o * 4 + i, (1 - s) * 8 + (o ^ a) * 4 + (i + b) % 4)
        for s in range(2)
        for o in range(2)
        for i in range(4)
    ]
    return lax.ppermute(v, ("section", "tp"), pairs)


def summed_in_steps(v):
    parts = [along_ring(v[b], "tp", b) for b in (1, 2, 3)]
    sums = [added(v[0][a], *(p[a] for p in parts)).astype(BF16) for a in range(2)]
    return [to_other(sums[a], a, 0) for a in range(2)]


def finished(main, tail, taken, rest, cot, owner):
    depth = cot.shape[1]
    parts = (*main, *tail)

    def kernel(own_ref, *refs):
        cot_ref, out, total = refs[-3:]
        for group, blocks in ((refs[: len(main)], taken), (refs[len(main) : -3], rest)):
            for i, b in enumerate(blocks):
                at = pl.ds(pl.multiple_of(own_ref[b] * PART, PART), PART)
                acc = cot_ref[at].astype(F32)
                for ref in group:
                    acc = acc + ref[i * PART : (i + 1) * PART].astype(F32)
                total[at] = acc
        out[...] = total[...].T.astype(BF16)

    return pl.pallas_call(
        kernel,
        out_shape=jax.ShapeDtypeStruct((depth, ROWS), BF16),
        grid_spec=pltpu.PrefetchScalarGridSpec(
            num_scalar_prefetch=1,
            grid=(1,),
            in_specs=[pl.BlockSpec(p.shape, lambda j, *_: (0, 0)) for p in (*parts, cot)],
            out_specs=pl.BlockSpec((depth, ROWS), lambda j, *_: (0, 0)),
            scratch_shapes=[pltpu.VMEM((ROWS, depth), F32)],
        ),
        cost_estimate=pl.CostEstimate(
            flops=9 * ROWS * depth, bytes_accessed=20 * ROWS * depth, transcendentals=0
        ),
        compiler_params=ROOM,
        name="finish",
    )(owner, *parts, cot)


def layers_back(normed, cotangent, w_gate, w_up, w_down):
    weights = (w_gate[0], w_up[0], w_down[0])
    columns = weights[0].shape[1]
    tiles = columns // TILE
    n_a = 5
    n_b = tiles - n_a
    scale = 1.0 / math.sqrt(8 * ROWS)

    me_f = lax.axis_index("fsdp")
    zh, y = me_f // 4, me_f % 4
    steps = jnp.arange(8, dtype=jnp.int32)
    turn = steps // 2 + steps // 4 - 2 * (steps // 6)
    owner = ((zh + steps % 2) % 2) * 4 + (y + turn) % 4 + held(weights[1:])
    own, cot_own = stacked(normed[0].T, cotangent[0].T)
    pieces = gathered(own)
    cot_other = to_other(cot_own, 0, 0)
    first, rest = range(6, 8), range(0, 6)
    rows, *b_first = project(pieces, owner, None, weights, first, n_a, n_b, TILE)
    a_first = project(None, None, rows, weights, first, 0, 2, n_a * TILE // 2)
    a_rest = project(None, None, rows, weights, rest, 0, n_a, TILE)
    b_rest = project(None, None, rows, weights, rest, n_a, n_b, TILE)
    sides = flipped(rows)

    def by_step(far, near):
        return [near[0:2], near[2:4], far, near[4:6]]

    a = spread_pair_first(activate(reduced_ring_first(by_step(a_first, a_rest))))
    b = spread_ring_first(activate(reduced_pair_first(by_step(b_first, b_rest))))

    def of(parts, group):
        return flat([parts[i] for i in group])

    def dx(group, earlier, final):
        return input_grad(of(a, group), of(b, group), weights[:2], n_a, n_b, earlier, final)

    groups = (0, 2, 4), (1, 3, 5), (6, 7)
    (part,) = dx(groups[0], None, False)
    main = summed_in_steps(dx(groups[1], part, True))
    sums_a = weight_sums(of(a, range(0, 6)), sides, n_a)
    sums_b = weight_sums(of(b, range(0, 5)), sides, n_b)
    tail = summed_in_steps(dx(groups[2], None, True))
    grads = weight_grads(of(a, range(6, 8)), sides, sums_a, 0, n_a, columns, scale, None)
    grads = weight_grads(of(b, range(5, 8)), sides, sums_b, n_a, n_b, columns, scale, grads)
    passed = finished(main, tail, groups[0] + groups[1], groups[2], cot_other, owner)
    return (passed.T[None], grads[0][None], grads[1][None], grads[2][None])


def solution(mesh):
    acts = P("section", "tp", "fsdp")
    weights = P("section", "fsdp", "tp")
    return jax.shard_map(
        layers_back,
        mesh=mesh,
        in_specs=(acts, acts, weights, weights, weights),
        out_specs=(acts, weights, weights, weights),
        check_vma=False,
    )
```
